256 devices in a mesh: band: 8 (over z_hi, y), grid: 32 (over z_lo, x, core).
Axes of the slice: x: 4, y: 4, z: 8 (z_hi: 2, z_lo: 4; z = z_hi * 4 + z_lo), core: 2. Of those that a mesh axis runs over, the one named last changes fastest.
Arguments:
- orbitals: bfloat16 [2048, 65536], P('band', 'grid'), as said below
- projectors: bfloat16 [2048, 65536], P('band', 'grid'), may hold values from -0.015625 to 0.015625
Outputs:
- result: bfloat16 [2048, 65536], P('band', 'grid')
- energies: float32 [2048], P('band')
The draws below stay inside these ranges and needn't reach their ends.
Inputs may be any that keep to these rules, and one draw needn't show every extreme that they name: The orbitals are real-valued.
All inputs are finite; a program needn't handle non-finite values.
Results may differ from the reference program's by a relative error of at most 0.0049.
Values may be sent and summed in bfloat16 or wider, within the bound.
A program may use at most 64 MiB of HBM per device.

```python
import jax
import jax.numpy as jnp
from jax import lax

NB = 2048
NG = 65536


def draw_orbitals(key, part):
    k_main = jax.random.fold_in(key, 11)
    k_rough = jax.random.fold_in(key, 12)
    place = jnp.arange(NG, dtype=jnp.float32) / (NG - 1)
    rising = 0.6 + 1.2 * place
    rough = jax.random.uniform(k_rough, (1, NG), jnp.float32, 0.5, 1.5)
    values = jax.random.normal(k_main, (NB, NG), jnp.float32)
    return (values * rising[None, :] * rough).astype(jnp.bfloat16)


def steps_of(rng, shape, pieces, smallest, top_value):
    factor_of = 1.0
    for dim, shards_of in pieces:
        steps = jax.random.uniform(jax.random.fold_in(jax.random.fold_in(rng, 6), dim), (shards_of,), jnp.float32, smallest / len(pieces), top_value / len(pieces))
        factor_of = factor_of * jnp.repeat(jnp.exp(steps), shape[dim] // shards_of).reshape((-1,) + (1,) * (len(shape) - 1 - dim))
    return factor_of


def normal_values(rng, dims, scale, limit, shards=(), kind=jnp.bfloat16):
    array = jax.random.normal(rng, dims, jnp.float32) * scale
    if len(shards) > 0:
        array = steps_of(rng, dims, shards, -0.22, 0.18) * array
    return jnp.clip(array, min=-limit, max=limit).astype(kind)


def setup_inputs(seed: int = 0) -> dict:
    splits = jax.random.split(jax.random.key(seed), 3)
    return {
        "orbitals": draw_orbitals(jax.random.fold_in(splits[2], 71), 0),
        "projectors": normal_values(splits[1], (NB, NG), (2 * NG) ** -0.5, 0.015625, ((0, 8), (1, 32))),
    }


def intersections(projectors, state):
    return jnp.dot(projectors.astype(jnp.float32), state.astype(jnp.float32).T, preferred_element_type=jnp.float32)


def update(projectors, state, rounded):
    widened = lax.optimization_barrier(rounded).astype(jnp.float32)
    return state.astype(jnp.float32) - jnp.dot(widened.T, projectors.astype(jnp.float32), preferred_element_type=jnp.float32)


def reference(orbitals, projectors):
    first = intersections(projectors, orbitals)
    first_b = first.astype(jnp.bfloat16)
    middle = update(projectors, orbitals, first_b).astype(jnp.bfloat16)
    second = intersections(projectors, middle)
    second_b = second.astype(jnp.bfloat16)
    result = update(projectors, middle, second_b).astype(jnp.bfloat16)
    wide = middle.astype(jnp.float32)
    norm = jnp.sum(wide * wide, axis=1)
    numer = jnp.sum(second * lax.optimization_barrier(second_b).astype(jnp.float32), axis=0)
    energies = (2.0 * NG / NB) * numer / norm
    return result, energies
```

```python
import functools

import jax
import jax.numpy as jnp
from jax import lax
from jax.experimental import pallas as pl
from jax.experimental.pallas import tpu as pltpu
from jax.sharding import PartitionSpec as P

MESH = pl.DeviceIdType.MESH
F32, BF16 = jnp.float32, jnp.bfloat16
NBLK = 8
CH = 4


def kernel(scale, psi_hbm, w_hbm, res, eout, wall, psi, psi1, acc, relay,
           xs, rc, xown, sx, bs, rx, sz, zs, rz, mbuf, mt, num, es, re,
           in_sem, w_send, yo, yf, zr, rl, zo, zf, s_send, s_recv, e_send, e_recv):
    rows, cols = psi.shape
    half = rows // 2
    crow = rows // CH
    b = lax.axis_index("band")
    g = lax.axis_index("grid")
    zh, y = b // 4, b % 4
    zl, x, c = g // 8, (g // 2) % 4, g % 2
    z = zh * 4 + zl

    def dev(zz, yy, xx, cc):
        return ((zz // 4) * 4 + yy, ((zz % 4) * 4 + xx) * 2 + cc)

    right, left = dev(z, (y + 1) % 4, x, c), dev(z, (y + 3) % 4, x, c)
    zup, zdn = dev((z + 2) % 8, y, x, c), dev((z + 6) % 8, y, x, c)
    mate = dev(z, y, x, 1 - c)
    xm = [(x + d) % 4 for d in (1, 2, 3)]
    zm = [(zl + d) % 4 for d in (1, 2, 3)]
    xdev = [dev(z, y, m, c) for m in xm]
    zdev = [dev(zh * 4 + m, y, x, c) for m in zm]

    def block(t):
        k = t % 4
        d = jnp.where(k == 1, 3, jnp.where(k == 2, 1, jnp.where(k == 3, 2, 0)))
        return ((zh + t // 4) % 2) * 4 + (y + d) % 4

    b_l, b_r, b_f = zh * 4 + (y + 3) % 4, zh * 4 + (y + 1) % 4, zh * 4 + (y + 2) % 4
    oz = 1 - zh
    z_o, z_l, z_r = oz * 4 + y, oz * 4 + (y + 3) % 4, oz * 4 + (y + 1) % 4
    z_f = oz * 4 + (y + 2) % 4

    def send(src, dst, ssem, rsem, to):
        pltpu.make_async_remote_copy(
            src_ref=src, dst_ref=dst, send_sem=ssem, recv_sem=rsem,
            device_id=to, device_id_type=MESH).start()

    def wait(ref, sem):
        pltpu.make_async_copy(ref, ref, sem).wait()

    def piece(blk, ch):
        return wall.at[blk, pl.ds(ch * crow, crow)]

    cw = pltpu.make_async_copy(w_hbm, wall.at[b], in_sem.at[0])
    cp = pltpu.make_async_copy(psi_hbm, psi, in_sem.at[1])
    cw.start()
    cp.start()

    barrier = pltpu.get_barrier_semaphore()
    peers = [right, left, zup, zdn, mate] + xdev + zdev
    for p in peers:
        pl.semaphore_signal(barrier, inc=1, device_id=p, device_id_type=MESH)
    acc[...] = jnp.zeros_like(acc)
    num[...] = jnp.zeros_like(num)
    es[...] = jnp.zeros_like(es)
    cw.wait()
    pl.semaphore_wait(barrier, len(peers))

    for cr, cl in ((0, 2), (1, 3), (2, 0), (3, 1)):
        send(piece(b, cr), piece(b, cr), w_send.at[0], yo.at[0, cr], right)
        send(piece(b, cl), piece(b, cl), w_send.at[0], yo.at[1, cl], left)
    for cu, cd in ((0, 2), (1, 3)):
        send(piece(b, cu), relay.at[cu], w_send.at[1], rl.at[cu], zup)
        send(piece(b, cd), relay.at[cd], w_send.at[1], rl.at[cd], zdn)
    cp.wait()

    def relay_on(ch):
        wait(relay.at[ch], rl.at[ch])
        if ch < 2:
            src = ((z + 6) % 8 // 4) * 4 + y
            send(relay.at[ch], piece(src, ch), w_send.at[2], zr.at[ch], zup)
        else:
            src = ((z + 2) % 8 // 4) * 4 + y
            send(relay.at[ch], piece(src, ch), w_send.at[2], zr.at[ch], zdn)

    def w_events(k):
        if k == 1:
            for cr, cl in ((0, 2), (1, 3)):
                wait(piece(b_l, cr), yo.at[0, cr])
                send(piece(b_l, cr), piece(b_l, cr), w_send.at[3], yf.at[cr], right)
                wait(piece(b_r, cl), yo.at[1, cl])
                send(piece(b_r, cl), piece(b_r, cl), w_send.at[3], yf.at[cl], left)
            relay_on(0)
            relay_on(2)
            wait(piece(b_l, 2), yo.at[0, 2])
            wait(piece(b_l, 3), yo.at[0, 3])
        elif k == 2:
            wait(piece(b_r, 0), yo.at[1, 0])
            wait(piece(b_r, 1), yo.at[1, 1])
            relay_on(1)
            relay_on(3)
        elif k == 3:
            wait(piece(b_f, 0), yf.at[0])
            wait(piece(b_f, 2), yf.at[2])
            for ch in (0, 2):
                wait(piece(z_o, ch), zr.at[ch])
                send(piece(z_o, ch), piece(z_o, ch), w_send.at[4], zo.at[0, ch], right)
                send(piece(z_o, ch), piece(z_o, ch), w_send.at[4], zo.at[1, ch], left)
            wait(piece(b_f, 1), yf.at[1])
            wait(piece(b_f, 3), yf.at[3])
        elif k == 4:
            for ch in (1, 3):
                wait(piece(z_o, ch), zr.at[ch])
                send(piece(z_o, ch), piece(z_o, ch), w_send.at[4], zo.at[0, ch], right)
                send(piece(z_o, ch), piece(z_o, ch), w_send.at[4], zo.at[1, ch], left)
        elif k == 5:
            for cr, cl in ((0, 2), (1, 3)):
                wait(piece(z_l, cr), zo.at[0, cr])
                send(piece(z_l, cr), piece(z_l, cr), w_send.at[5], zf.at[cr], right)
                wait(piece(z_r, cl), zo.at[1, cl])
                send(piece(z_r, cl), piece(z_r, cl), w_send.at[5], zf.at[cl], left)
            wait(piece(z_l, 2), zo.at[0, 2])
            wait(piece(z_l, 3), zo.at[0, 3])
        elif k == 6:
            wait(piece(z_r, 0), zo.at[1, 0])
            wait(piece(z_r, 1), zo.at[1, 1])
        elif k == 7:
            for ch in (0, 2, 1, 3):
                wait(piece(z_f, ch), zf.at[ch])

    def stage_a(p, t):
        state = psi if p == 0 else psi1
        v = lax.dot_general(wall[block(t)], state[...], (((1,), (1,)), ((), ())),
                            preferred_element_type=F32)
        lo, hi = v[:, :half], v[:, half:]
        xown[t] = jnp.where(c == 0, lo, hi)
        xs[p, t] = jnp.where(c == 0, hi, lo).astype(BF16)
        send(xs.at[p, t], rc.at[p, t], s_send.at[p, 0], s_recv.at[p, 0, t], mate)

    def stage_b(p, t):
        wait(rc.at[p, t], s_recv.at[p, 0, t])
        s = (xown[t] + rc[p, t].astype(F32)).reshape(4, rows // 4, half)
        bs[t] = s
        sx[p, t] = s.astype(BF16)
        for d in range(3):
            send(sx.at[p, t, xm[d]], rx.at[p, t, d], s_send.at[p, 1],
                 s_recv.at[p, 1, t], xdev[d])

    def stage_c(p, t):
        wait(rx.at[p, t], s_recv.at[p, 1, t])
        s = bs[t, x]
        for d in range(3):
            s = s + rx[p, t, d].astype(F32)
        s = s.reshape(4, rows // 16, half)
        zs[t] = s
        sz[p, t] = s.astype(BF16)
        for d in range(3):
            send(sz.at[p, t, zm[d]], rz.at[p, t, d], s_send.at[p, 2],
                 s_recv.at[p, 2, t], zdev[d])

    def stage_d(p, t):
        wait(rz.at[p, t], s_recv.at[p, 2, t])
        s = zs[t, zl]
        for d in range(3):
            s = s + rz[p, t, d].astype(F32)
        r = s.astype(BF16)
        mine = mbuf.at[p, c, block(t), x, zl]
        mine[...] = r
        if p == 1:
            num[...] += jnp.sum(s * r.astype(F32), axis=0, keepdims=True)
        for d in range(3):
            send(mine, mine, s_send.at[p, 3], s_recv.at[p, 3, t], zdev[d])

    def stage_e(p, t):
        wait(rz.at[p, t], s_recv.at[p, 3, t])
        mine = mbuf.at[p, c, block(t), x]
        for d in range(3):
            send(mine, mine, s_send.at[p, 4], s_recv.at[p, 4, t], xdev[d])

    def stage_f(p, t):
        wait(rx.at[p, t], s_recv.at[p, 4, t])
        mine = mbuf.at[p, c, block(t)]
        send(mine, mine, s_send.at[p, 5], s_recv.at[p, 5, t], mate)

    def stage_g(p, t):
        wait(rc.at[p, t], s_recv.at[p, 5, t])
        blk = block(t)
        for h in range(2):
            m = mbuf[p, h, blk].reshape(rows, half).astype(F32)
            mt[pl.ds(h * half, half), :] = m.T.astype(BF16)
        width = 512

        def part(i, carry):
            at = pl.ds(pl.multiple_of(i * width, width), width)
            acc[:, at] += jnp.dot(mt[...], wall[blk, :, at], preferred_element_type=F32)
            return carry

        lax.fori_loop(0, cols // width, part, 0)

    stages = (stage_a, stage_b, stage_c, stage_d, stage_e, stage_f, stage_g)

    def tick(T, carry):
        for k in range(1, 7):
            @pl.when(T == k)
            def _(k=k):
                w_events(k)

        for s in (6, 5, 4, 3, 2, 1):
            u = T - s

            @pl.when(((u >= 0) & (u <= 6)) | (u == 10))
            def _(s=s, u=u):
                stages[s](0, jnp.minimum(u, 7))

        @pl.when(T == 10)
        def _():
            w_events(7)

        @pl.when((T <= 6) | (T == 10))
        def _():
            stage_a(0, jnp.minimum(T, 7))

        return carry

    lax.fori_loop(0, 17, tick, 0)

    step = 64

    def first(i, carry):
        at = pl.ds(pl.multiple_of(i * step, step), step)
        v = (psi[at, :].astype(F32) - acc[at, :]).astype(BF16)
        psi1[at, :] = v
        acc[at, :] = jnp.zeros((step, cols), F32)
        w = v.astype(F32)
        n = jnp.sum(w * w, axis=1, keepdims=True)
        mtn = jnp.broadcast_to(n, (step, half))
        xown[0, at, :] = mtn
        return carry

    lax.fori_loop(0, rows // step, first, 0)
    for h in range(2):
        es[0, pl.ds(1 + h, 1), :] = xown[0, pl.ds(h * half, half), :].T[0:1, :]

    def run(s):
        def body(t, carry):
            stages[s](1, t)
            return carry

        lax.fori_loop(0, NBLK, body, 0)

    for s in range(4):
        run(s)
    es[0, 0:1, :] = num[...]
    for d in range(3):
        send(es.at[0], re.at[0, d], e_send.at[0], e_recv.at[0], zdev[d])
    run(4)
    wait(re.at[0], e_recv.at[0])
    es[1] = es[0] + re[0, 0] + re[0, 1] + re[0, 2]
    for d in range(3):
        send(es.at[1], re.at[1, d], e_send.at[1], e_recv.at[1], xdev[d])
    run(5)
    wait(re.at[1], e_recv.at[1])
    es[2] = es[1] + re[1, 0] + re[1, 1] + re[1, 2]
    send(es.at[2], re.at[2, 0], e_send.at[2], e_recv.at[2], mate)
    run(6)

    def last(i, carry):
        at = pl.ds(pl.multiple_of(i * step, step), step)
        res[at, :] = (psi1[at, :].astype(F32) - acc[at, :]).astype(BF16)
        return carry

    lax.fori_loop(0, rows // step, last, 0)

    wait(re.at[2, 0], e_recv.at[2])
    own, other = es[2, 0:1, :], re[2, 0, 0:1, :]
    lo = jnp.where(c == 0, own, other)
    hi = jnp.where(c == 0, other, own)
    norm = es[2, 1:3, :] + re[2, 0, 1:3, :]
    eout[0:1, :] = scale * lo / norm[0:1]
    eout[1:2, :] = scale * hi / norm[1:2]

    wait(wall.at[pl.ds(0, 2)], w_send.at[0])
    wait(wall.at[0], w_send.at[1])
    wait(wall.at[0], w_send.at[2])
    wait(wall.at[0], w_send.at[3])
    wait(wall.at[pl.ds(0, 2)], w_send.at[4])
    wait(wall.at[0], w_send.at[5])
    for p in range(2):
        for k, ref in enumerate((rc, rx, rz, rz, rx, rc)):
            wait(ref.at[p], s_send.at[p, k])
    wait(re.at[0], e_send.at[0])
    wait(re.at[1], e_send.at[1])
    wait(re.at[2, 0], e_send.at[2])


def per_device(orbitals, projectors):
    rows, cols = orbitals.shape
    half, crow = rows // 2, rows // CH
    bands = rows * lax.axis_size("band")
    points = cols * lax.axis_size("grid")
    dma = pltpu.SemaphoreType.DMA
    vmem = pltpu.VMEM
    result, energies = pl.pallas_call(
        functools.partial(kernel, 2.0 * points / bands),
        out_shape=(jax.ShapeDtypeStruct((rows, cols), BF16),
                   jax.ShapeDtypeStruct((2, half), F32)),
        in_specs=[pl.BlockSpec(memory_space=pl.ANY)] * 2,
        out_specs=(pl.BlockSpec(memory_space=pltpu.VMEM),
                   pl.BlockSpec(memory_space=pltpu.VMEM)),
        scratch_shapes=[
            vmem((NBLK, rows, cols), BF16),
            vmem((rows, cols), BF16),
            vmem((rows, cols), BF16),
            vmem((rows, cols), F32),
            vmem((CH, crow, cols), BF16),
            vmem((2, NBLK, rows, half), BF16),
            vmem((2, NBLK, rows, half), BF16),
            vmem((NBLK, rows, half), F32),
            vmem((2, NBLK, 4, rows // 4, half), BF16),
            vmem((NBLK, 4, rows // 4, half), F32),
            vmem((2, NBLK, 3, rows // 4, half), BF16),
            vmem((2, NBLK, 4, rows // 16, half), BF16),
            vmem((NBLK, 4, rows // 16, half), F32),
            vmem((2, NBLK, 3, rows // 16, half), BF16),
            vmem((2, 2, NBLK, 4, 4, rows // 16, half), BF16),
            vmem((rows, rows), BF16),
            vmem((1, half), F32),
            vmem((3, 8, half), F32),
            vmem((3, 3, 8, half), F32),
            dma((2,)),
            dma((6,)),
            dma((2, CH)),
            dma((CH,)),
            dma((CH,)),
            dma((CH,)),
            dma((2, CH)),
            dma((CH,)),
            dma((2, 6)),
            dma((2, 6, NBLK)),
            dma((3,)),
            dma((3,)),
        ],
        compiler_params=pltpu.CompilerParams(
            collective_id=0, has_side_effects=True, vmem_limit_bytes=60_000_000),
    )(orbitals, projectors)
    return result, energies.reshape(rows)


def solution(mesh):
    in_specs = (P("band", "grid"), P("band", "grid"))
    out_specs = (P("band", "grid"), P("band"))
    return jax.shard_map(
        per_device, mesh=mesh, in_specs=in_specs, out_specs=out_specs, check_vma=False
    )
```

```python
import functools

import jax
import jax.numpy as jnp
from jax import lax
from jax.experimental import pallas as pl
from jax.experimental.pallas import tpu as pltpu
from jax.sharding import PartitionSpec as P

MESH = pl.DeviceIdType.MESH
F32, BF16 = jnp.float32, jnp.bfloat16
CH = 4
NU = 8
NT = (((1,), (1,)), ((), ()))


def kernel(scale, psi_hbm, w_hbm, res, eout, wall, st, psi1, acc,
           xs, rc, xown, sx, bs, rx, sz, zs, rz, m1f, mbuf, sg, mt, mt2, nrm, es, re,
           in_sem, w_send, n_recv, f_recv, z_recv, s_send, c_recv, x_recv, zz_recv,
           gz_recv, gx_recv, gc_recv, sr_recv, sc_recv, hz_recv, hx_recv, hc_recv,
           e_send, e_recv):
    rows, cols = psi1.shape
    half = rows // 2
    crow = rows // CH
    b = lax.axis_index("band")
    g = lax.axis_index("grid")
    zh, y = b // 4, b % 4
    zl, x, c = g // 8, (g // 2) % 4, g % 2

    def dev(hh, yy, ll, xx, cc):
        return (hh * 4 + yy, (ll * 4 + xx) * 2 + cc)

    ym = [(y + d) % 4 for d in (1, 3, 2)]
    xm = [(x + d) % 4 for d in (1, 2, 3)]
    zm = [(zl + d) % 4 for d in (1, 2, 3)]
    ydev = [dev(zh, m, zl, x, c) for m in ym]
    odev = [dev(1 - zh, m, zl, x, c) for m in ym]
    right, left = ydev[0], ydev[1]
    zpart = dev(1 - zh, y, zl, x, c)
    mate = dev(zh, y, zl, x, 1 - c)
    xdev = [dev(zh, y, zl, m, c) for m in xm]
    zdev = [dev(zh, y, m, x, c) for m in zm]

    def unit(t):
        return (t % 4) * 2 + (zh + t // 4) % 2

    def send(src, dst, ssem, rsem, to):
        pltpu.make_async_remote_copy(
            src_ref=src, dst_ref=dst, send_sem=ssem, recv_sem=rsem,
            device_id=to, device_id_type=MESH).start()

    def wait(ref, sem):
        pltpu.make_async_copy(ref, ref, sem).wait()

    own = [wall.at[ch * 2 + zh, y] for ch in range(CH)]
    loads = [pltpu.make_async_copy(w_hbm.at[pl.ds(ch * crow, crow)], own[ch], in_sem.at[ch])
             for ch in range(CH)]
    loads.append(pltpu.make_async_copy(psi_hbm, st.at[pl.ds(0, rows)], in_sem.at[CH]))
    loads.append(pltpu.make_async_copy(w_hbm, st.at[pl.ds(rows, rows)], in_sem.at[CH + 1]))
    for load in loads:
        load.start()

    barrier = pltpu.get_barrier_semaphore()
    peers = ydev + odev + [zpart, mate] + xdev + zdev
    for p in peers:
        pl.semaphore_signal(barrier, inc=1, device_id=p, device_id_type=MESH)
    acc[...] = jnp.zeros_like(acc)
    es[...] = jnp.zeros_like(es)
    for load in loads:
        load.wait()
    pl.semaphore_wait(barrier, len(peers))

    for ch in range(CH):
        send(own[ch], own[ch], w_send.at[1], z_recv.at[ch], zpart)

    def near(k):
        piece = wall.at[unit(k), y]
        send(piece, piece, w_send.at[0], n_recv.at[0, k], right)
        send(piece, piece, w_send.at[0], n_recv.at[1, k], left)

    near(0)
    near(1)

    def pass_on(k):
        for side, m, to in ((0, (y + 3) % 4, right), (1, (y + 1) % 4, left)):
            wait(wall.at[0, 0], n_recv.at[side, k])
            part = wall.at[unit(k), m, pl.ds(side * (crow // 2), crow // 2)]
            send(part, part, w_send.at[2], f_recv.at[k], to)

        @pl.when((k + 2 >= CH) & (k + 2 < NU))
        def _():
            wait(wall.at[0, 0], z_recv.at[k + 2 - CH])

        @pl.when(k + 2 < NU)
        def _():
            near(k + 2)

    def stage_a(t):
        v = lax.dot_general(wall[unit(t)].reshape(rows, cols), st[...], NT,
                            preferred_element_type=F32)
        q = [v[:, i * half:(i + 1) * half] for i in range(4)]
        for i in range(2):
            at = slice(i * half, (i + 1) * half)
            xown[:, at] = jnp.where(c == 0, q[2 * i], q[2 * i + 1])
            xs[t, :, at] = jnp.where(c == 0, q[2 * i + 1], q[2 * i]).astype(BF16)
        send(xs.at[t], rc.at[t], s_send.at[0], c_recv.at[t], mate)

    def stage_b(t):
        wait(rc.at[t], c_recv.at[t])
        s = (xown[...] + rc[t].astype(F32)).reshape(4, crow, rows)
        bs[...] = s
        sx[t] = s.astype(BF16)
        for d in range(3):
            send(sx.at[t, xm[d]], rx.at[t, d], s_send.at[1], x_recv.at[t], xdev[d])

    def stage_c(t):
        wait(rx.at[t], x_recv.at[t])
        s = bs[x]
        for d in range(3):
            s = s + rx[t, d].astype(F32)
        s = s.reshape(4, crow // 4, rows)
        zs[t] = s
        sz[t] = s.astype(BF16)
        for d in range(3):
            send(sz.at[t, zm[d]], rz.at[t, d], s_send.at[2], zz_recv.at[t], zdev[d])

    def stage_d(t):
        wait(rz.at[t], zz_recv.at[t])
        s = zs[t, zl]
        for d in range(3):
            s = s + rz[t, d].astype(F32)
        u = unit(t)
        m1f[u] = s[:, :half]
        mine, mys = mbuf.at[0, c, u, x, zl], sg.at[c, u, b]
        mine[...] = s[:, :half].astype(BF16)
        mys[...] = s[:, half:].astype(BF16)
        for d in range(3):
            send(mine, mine, s_send.at[3], gz_recv.at[t], zdev[d])
        for to in odev + [zpart] + ydev:
            send(mys, mys, s_send.at[6], sr_recv.at[u], to)

    def stage_e(t):
        wait(mbuf.at[0, 0, 0, 0, pl.ds(0, 3)], gz_recv.at[t])
        mine = mbuf.at[0, c, unit(t), x]
        for d in range(3):
            send(mine, mine, s_send.at[4], gx_recv.at[t], xdev[d])

    def stage_f(t):
        wait(mbuf.at[0, 0, 0, pl.ds(0, 3)], gx_recv.at[t])
        mine = mbuf.at[0, c, unit(t)]
        send(mine, mine, s_send.at[5], gc_recv.at[t], mate)

    width = 512

    def stage_g(t):
        wait(mbuf.at[0, 0, 0], gc_recv.at[t])
        u = unit(t)
        for h in range(2):
            m = mbuf[0, h, u].reshape(rows, half).astype(F32)
            mt[pl.ds(h * half, half), :] = m.T.astype(BF16)

        def part(i, carry):
            at = pl.ds(pl.multiple_of(i * width, width), width)
            acc[:, at] += jnp.dot(mt[...], wall[u, :, :, at].reshape(rows, width),
                                  preferred_element_type=F32)
            return carry

        lax.fori_loop(0, cols // width, part, 0)

    late = 5

    def done(t):
        return jnp.where(t < late, 0, t - 1)

    def over(stage, lo, hi):
        def body(t, carry):
            stage(t)
            return carry

        lax.fori_loop(lo, hi, body, 0)

    def tick(n, carry):
        @pl.when(n < NU)
        def _():
            pass_on(n)

        t = n - 1
        two, one, now = done(t - 2), done(t - 1), done(t)

        @pl.when(t >= 1)
        def _():
            stage_c(t - 1)

        over(stage_d, one, now)
        over(stage_f, two, one)

        @pl.when(t >= 0)
        def _():
            wait(wall.at[0, 0], f_recv.at[t])
            stage_a(t)

        @pl.when(t >= 0)
        def _():
            stage_b(t)

        over(stage_e, one, now)
        over(stage_g, jnp.where(t == NU - 2, 0, 2), 2)
        return carry

    lax.fori_loop(0, NU + 1, tick, 0)
    stage_d(NU - 2)
    over(stage_g, 2, 4)
    stage_c(NU - 1)
    stage_f(NU - 3)
    stage_e(NU - 2)
    over(stage_g, 4, 6)
    stage_d(NU - 1)
    early = NU - 2
    for u in range(early):
        wait(sg.at[0, 0, pl.ds(0, 7)], sr_recv.at[u])
    send(sg.at[c, pl.ds(0, early)], sg.at[c, pl.ds(0, early)], s_send.at[7], sc_recv.at[0], mate)
    stage_f(NU - 2)
    stage_g(NU - 2)
    stage_e(NU - 1)
    for u in range(early, NU):
        wait(sg.at[0, 0, pl.ds(0, 7)], sr_recv.at[u])
    send(sg.at[c, pl.ds(early, 2)], sg.at[c, pl.ds(early, 2)], s_send.at[7], sc_recv.at[1], mate)
    stage_f(NU - 1)
    wait(sg.at[0, pl.ds(0, early)], sc_recv.at[0])
    wait(sg.at[0, pl.ds(0, 2)], sc_recv.at[1])

    m2 = m1f[...].reshape(NU * crow // 4, half)
    for o in range(8):
        for h in range(2):
            k = [mbuf[0, c, (2 * h + i) * 2 + o // 4, o % 4].reshape(crow, half)
                 for i in range(2)]
            m2 = m2 - jnp.dot(sg[h, :, o].reshape(NU * crow // 4, half),
                              jnp.concatenate(k, axis=0), preferred_element_type=F32)
    r = m2.astype(BF16)
    es[0, 0:1, :] = jnp.sum(m2 * r.astype(F32), axis=0, keepdims=True)
    share = crow // 4
    for u in range(NU):
        mbuf[1, c, u, x, zl] = r[u * share:(u + 1) * share]
    NP = 4
    for p in range(NP):
        mine = mbuf.at[1, c, pl.ds(2 * p, 2), x, zl]
        for d in range(3):
            send(mine, mine, s_send.at[8], hz_recv.at[p], zdev[d])

    stage_g(NU - 1)
    step = 64

    def first(i, carry):
        at = pl.ds(pl.multiple_of(i * step, step), step)
        v = (st[at, :].astype(F32) - acc[at, :]).astype(BF16)
        psi1[at, :] = v
        w = v.astype(F32)
        n = jnp.sum(w * w, axis=1, keepdims=True)
        nrm[at, :] = jnp.broadcast_to(n, (step, half))
        return carry

    lax.fori_loop(0, rows // step, first, 0)
    for h in range(2):
        es[0, pl.ds(1 + h, 1), :] = nrm[pl.ds(h * half, half), :].T[0:1, :]
    for d in range(3):
        send(es.at[0], re.at[0, d], e_send.at[0], e_recv.at[0], zdev[d])
    for p in range(NP):
        wait(mbuf.at[0, 0, pl.ds(0, 2), 0, pl.ds(0, 3)], hz_recv.at[p])
        mine = mbuf.at[1, c, pl.ds(2 * p, 2), x]
        for d in range(3):
            send(mine, mine, s_send.at[9], hx_recv.at[p], xdev[d])
    wait(re.at[0], e_recv.at[0])
    es[1] = es[0] + re[0, 0] + re[0, 1] + re[0, 2]
    for d in range(3):
        send(es.at[1], re.at[1, d], e_send.at[1], e_recv.at[1], xdev[d])

    def turn(p, h):
        for u in (2 * p, 2 * p + 1):
            m = mbuf[1, h, u].reshape(rows, half).astype(F32)
            mt2[pl.ds(pl.multiple_of(h * half, half), half), u * rows:(u + 1) * rows] = (
                m.T.astype(BF16))

    for p in range(NP):
        wait(mbuf.at[0, 0, pl.ds(0, 2), pl.ds(0, 3)], hx_recv.at[p])
        mine = mbuf.at[1, c, pl.ds(2 * p, 2)]
        send(mine, mine, s_send.at[10], hc_recv.at[p], mate)
        turn(p, c)
    wait(re.at[1], e_recv.at[1])
    es[2] = es[1] + re[1, 0] + re[1, 1] + re[1, 2]
    send(es.at[2], re.at[2, 0], e_send.at[2], e_recv.at[2], mate)
    for p in range(NP):
        wait(mbuf.at[0, 0, pl.ds(0, 2)], hc_recv.at[p])
        turn(p, 1 - c)

    def last(i, carry):
        at = pl.ds(pl.multiple_of(i * width, width), width)
        change = jnp.dot(mt2[...], wall[:, :, :, at].reshape(NU * rows, width),
                         preferred_element_type=F32)
        res[:, at] = (psi1[:, at].astype(F32) - change).astype(BF16)
        return carry

    lax.fori_loop(0, cols // width, last, 0)

    wait(re.at[2, 0], e_recv.at[2])
    mine, other = es[2, 0:1, :], re[2, 0, 0:1, :]
    norm = es[2, 1:3, :] + re[2, 0, 1:3, :]
    eout[0:1, :] = scale * jnp.where(c == 0, mine, other) / norm[0:1]
    eout[1:2, :] = scale * jnp.where(c == 0, other, mine) / norm[1:2]

    wait(wall.at[pl.ds(0, 4)], w_send.at[0])
    wait(wall.at[0], w_send.at[1])
    wait(wall.at[pl.ds(0, 2)], w_send.at[2])
    sizes = (rc, rx, rz, mbuf.at[0, 0, :, 0, pl.ds(0, 3)], mbuf.at[0, 0, :, pl.ds(0, 3)],
             mbuf.at[0, 0], sg.at[0, :, pl.ds(0, 7)], sg.at[0],
             mbuf.at[0, 0, :, 0, pl.ds(0, 3)], mbuf.at[0, 0, :, pl.ds(0, 3)], mbuf.at[0, 0])
    for k, ref in enumerate(sizes):
        wait(ref, s_send.at[k])
    wait(re.at[0], e_send.at[0])
    wait(re.at[1], e_send.at[1])
    wait(re.at[2, 0], e_send.at[2])


def per_device(orbitals, projectors):
    rows, cols = orbitals.shape
    half, crow = rows // 2, rows // CH
    share = crow // 4
    bands = rows * lax.axis_size("band")
    points = cols * lax.axis_size("grid")
    dma = pltpu.SemaphoreType.DMA
    vmem = pltpu.VMEM
    result, energies = pl.pallas_call(
        functools.partial(kernel, 2.0 * points / bands),
        out_shape=(jax.ShapeDtypeStruct((rows, cols), BF16),
                   jax.ShapeDtypeStruct((2, half), F32)),
        in_specs=[pl.BlockSpec(memory_space=pl.ANY)] * 2,
        out_specs=(pl.BlockSpec(memory_space=pltpu.VMEM),
                   pl.BlockSpec(memory_space=pltpu.VMEM)),
        scratch_shapes=[
            vmem((NU, 4, crow, cols), BF16),
            vmem((2 * rows, cols), BF16),
            vmem((rows, cols), BF16),
            vmem((rows, cols), F32),
            vmem((NU, rows, rows), BF16),
            vmem((NU, rows, rows), BF16),
            vmem((rows, rows), F32),
            vmem((NU, 4, crow, rows), BF16),
            vmem((4, crow, rows), F32),
            vmem((NU, 3, crow, rows), BF16),
            vmem((NU, 4, share, rows), BF16),
            vmem((NU, 4, share, rows), F32),
            vmem((NU, 3, share, rows), BF16),
            vmem((NU, share, half), F32),
            vmem((2, 2, NU, 4, 4, share, half), BF16),
            vmem((2, NU, 8, share, half), BF16),
            vmem((rows, rows), BF16),
            vmem((rows, NU * rows), BF16),
            vmem((rows, half), F32),
            vmem((3, 8, half), F32),
            vmem((3, 3, 8, half), F32),
            dma((CH + 2,)),
            dma((3,)),
            dma((2, NU)),
            dma((NU,)),
            dma((CH,)),
            dma((11,)),
            dma((NU,)),
            dma((NU,)),
            dma((NU,)),
            dma((NU,)),
            dma((NU,)),
            dma((NU,)),
            dma((NU,)),
            dma((2,)),
            dma((4,)),
            dma((4,)),
            dma((4,)),
            dma((3,)),
            dma((3,)),
        ],
        compiler_params=pltpu.CompilerParams(
            collective_id=0, has_side_effects=True, vmem_limit_bytes=60_000_000),
    )(orbitals, projectors)
    return result, energies.reshape(rows)


def solution(mesh):
    in_specs = (P("band", "grid"), P("band", "grid"))
    out_specs = (P("band", "grid"), P("band"))
    return jax.shard_map(
        per_device, mesh=mesh, in_specs=in_specs, out_specs=out_specs, check_vma=False
    )
```

```python
import functools

import jax
import jax.numpy as jnp
from jax import lax
from jax.experimental import pallas as pl
from jax.experimental.pallas import tpu as pltpu
from jax.sharding import PartitionSpec as P

MESH = pl.DeviceIdType.MESH
F32, BF16 = jnp.float32, jnp.bfloat16
CH = 4
NU = 8
NT = (((1,), (1,)), ((), ()))


def kernel(scale, psi_hbm, w_hbm, res, eout, wall, st, psi1, acc,
           xs, rc, xown, sx, bs, rx, sz, zs, rz, m1f, mbuf, sg, mt, mt2, nrm, es, re,
           in_sem, w_send, n_recv, m_recv, f_recv, z_recv, s_send, c_recv, x_recv, zz_recv,
           gz_recv, gx_recv, gc_recv, sr_recv, sc_recv, hz_recv, hx_recv, hc_recv,
           e_send, e_recv):
    rows, cols = psi1.shape
    half = rows // 2
    crow = rows // CH
    b = lax.axis_index("band")
    g = lax.axis_index("grid")
    zh, y = b // 4, b % 4
    zl, x, c = g // 8, (g // 2) % 4, g % 2

    def dev(hh, yy, ll, xx, cc):
        return (hh * 4 + yy, (ll * 4 + xx) * 2 + cc)

    ym = [(y + d) % 4 for d in (1, 3, 2)]
    xm = [(x + d) % 4 for d in (1, 2, 3)]
    zm = [(zl + d) % 4 for d in (1, 2, 3)]
    ydev = [dev(zh, m, zl, x, c) for m in ym]
    odev = [dev(1 - zh, m, zl, x, c) for m in ym]
    right, left = ydev[0], ydev[1]
    zpart = dev(1 - zh, y, zl, x, c)
    mate = dev(zh, y, zl, x, 1 - c)
    xdev = [dev(zh, y, zl, m, c) for m in xm]
    zdev = [dev(zh, y, m, x, c) for m in zm]

    def unit(t):
        return (t % 4) * 2 + (zh + t // 4) % 2

    def send(src, dst, ssem, rsem, to):
        pltpu.make_async_remote_copy(
            src_ref=src, dst_ref=dst, send_sem=ssem, recv_sem=rsem,
            device_id=to, device_id_type=MESH).start()

    def wait(ref, sem):
        pltpu.make_async_copy(ref, ref, sem).wait()

    barrier = pltpu.get_barrier_semaphore()
    peers = odev + [zpart] + zdev + ydev + xdev + [mate]
    for p in peers:
        pl.semaphore_signal(barrier, inc=1, device_id=p, device_id_type=MESH)
    own = [wall.at[ch * 2 + zh, y] for ch in range(CH)]
    loads = [pltpu.make_async_copy(w_hbm.at[pl.ds(ch * crow, crow)], own[ch], in_sem.at[ch])
             for ch in range(CH)]
    loads.append(pltpu.make_async_copy(psi_hbm, st.at[pl.ds(0, rows)], in_sem.at[CH]))
    loads.append(pltpu.make_async_copy(w_hbm, st.at[pl.ds(rows, rows)], in_sem.at[CH + 1]))
    for load in loads:
        load.start()
    for load in loads[:CH]:
        load.wait()
    pl.semaphore_wait(barrier, len(peers))

    for ch in range(CH):
        send(own[ch], own[ch], w_send.at[1], z_recv.at[ch], zpart)

    hrow = crow // 2

    def near(k, kept):
        for side, to in ((0, right), (1, left)):
            part = wall.at[unit(k), y, pl.ds((side ^ kept) * hrow, hrow)]
            sem = m_recv.at[k] if kept else n_recv.at[side, k]
            send(part, part, w_send.at[0], sem, to)

    def pass_on(k):
        for side, m, to in ((0, (y + 3) % 4, right), (1, (y + 1) % 4, left)):
            wait(wall.at[0, 0, pl.ds(0, hrow)], n_recv.at[side, k])
            part = wall.at[unit(k), m, pl.ds(side * hrow, hrow)]
            send(part, part, w_send.at[2], f_recv.at[k], to)

        @pl.when(k + 1 < NU)
        def _():
            near(k + 1, 1)

        @pl.when((k + 2 >= CH) & (k + 2 < NU))
        def _():
            wait(wall.at[0, 0], z_recv.at[k + 2 - CH])

        @pl.when(k + 2 < NU)
        def _():
            near(k + 2, 0)

    near(0, 0)
    near(0, 1)
    near(1, 0)
    acc[...] = jnp.zeros_like(acc)
    es[...] = jnp.zeros_like(es)
    for load in loads[CH:]:
        load.wait()

    def stage_a(t):
        v = lax.dot_general(wall[unit(t)].reshape(rows, cols), st[...], NT,
                            preferred_element_type=F32)
        q = [v[:, i * half:(i + 1) * half] for i in range(4)]
        for i in range(2):
            at = slice(i * half, (i + 1) * half)
            xown[:, at] = jnp.where(c == 0, q[2 * i], q[2 * i + 1])
            xs[t, :, at] = jnp.where(c == 0, q[2 * i + 1], q[2 * i]).astype(BF16)
        send(xs.at[t], rc.at[t], s_send.at[0], c_recv.at[t], mate)

    def stage_b(t):
        wait(rc.at[t], c_recv.at[t])
        s = (xown[...] + rc[t].astype(F32)).reshape(4, crow, rows)
        bs[t % 2] = s
        sx[t] = s.astype(BF16)
        for d in range(3):
            send(sx.at[t, xm[d]], rx.at[t, d], s_send.at[1], x_recv.at[t], xdev[d])

    def stage_c(t):
        wait(rx.at[t], x_recv.at[t])
        s = bs[t % 2, x]
        for d in range(3):
            s = s + rx[t, d].astype(F32)
        s = s.reshape(4, crow // 4, rows)
        zs[t] = s
        sz[t] = s.astype(BF16)
        for d in range(3):
            send(sz.at[t, zm[d]], rz.at[t, d], s_send.at[2], zz_recv.at[t], zdev[d])

    def stage_d(t):
        wait(rz.at[t], zz_recv.at[t])
        s = zs[t, zl]
        for d in range(3):
            s = s + rz[t, d].astype(F32)
        u = unit(t)
        m1f[u] = s[:, :half]
        mine, mys = mbuf.at[0, c, u, x, zl], sg.at[c, u, b]
        mine[...] = s[:, :half].astype(BF16)
        mys[...] = s[:, half:].astype(BF16)
        for d in range(3):
            send(mine, mine, s_send.at[3], gz_recv.at[t], zdev[d])
        for to in odev + [zpart] + ydev:
            send(mys, mys, s_send.at[6], sr_recv.at[u], to)

    def stage_e(t):
        wait(mbuf.at[0, 0, 0, 0, pl.ds(0, 3)], gz_recv.at[t])
        mine = mbuf.at[0, c, unit(t), x]
        for d in range(3):
            send(mine, mine, s_send.at[4], gx_recv.at[t], xdev[d])

    def stage_f(t):
        wait(mbuf.at[0, 0, 0, pl.ds(0, 3)], gx_recv.at[t])
        mine = mbuf.at[0, c, unit(t)]
        send(mine, mine, s_send.at[5], gc_recv.at[t], mate)

    width = 512

    def stage_g(t):
        wait(mbuf.at[0, 0, 0], gc_recv.at[t])
        u = unit(t)
        for h in range(2):
            m = mbuf[0, h, u].reshape(rows, half).astype(F32)
            mt[pl.ds(h * half, half), :] = m.T.astype(BF16)

        def part(i, carry):
            at = pl.ds(pl.multiple_of(i * width, width), width)
            acc[:, at] += jnp.dot(mt[...], wall[u, :, :, at].reshape(rows, width),
                                  preferred_element_type=F32)
            return carry

        lax.fori_loop(0, cols // width, part, 0)

    late = 4

    def done(t):
        return jnp.where(t < late, 0, t - 1)

    def over(stage, lo, hi):
        def body(t, carry):
            stage(t)
            return carry

        lax.fori_loop(lo, hi, body, 0)

    def tick(n, carry):
        @pl.when(n < NU)
        def _():
            pass_on(n)

        t = n - 1

        @pl.when(t >= 0)
        def _():
            wait(wall.at[0, 0], m_recv.at[t])
            wait(wall.at[0, 0], f_recv.at[t])
            stage_a(t)

        @pl.when(t >= 0)
        def _():
            stage_b(t)

        @pl.when(t >= 1)
        def _():
            stage_c(t - 1)

        over(stage_d, done(t - 1), done(t))
        over(stage_e, done(t - 2), done(t - 1))
        over(stage_f, done(t - 3), done(t - 2))
        return carry

    lax.fori_loop(0, NU + 1, tick, 0)
    stage_g(0)
    stage_c(NU - 1)
    stage_e(NU - 3)
    stage_f(NU - 4)
    stage_g(1)
    stage_d(NU - 2)
    stage_g(2)
    stage_d(NU - 1)
    stage_f(NU - 3)
    stage_g(3)
    stage_e(NU - 2)
    early = NU - 2
    for u in range(early):
        wait(sg.at[0, 0, pl.ds(0, 7)], sr_recv.at[u])
    send(sg.at[c, pl.ds(0, early)], sg.at[c, pl.ds(0, early)], s_send.at[7], sc_recv.at[0], mate)
    stage_g(4)
    stage_e(NU - 1)
    stage_f(NU - 2)
    stage_g(5)
    for u in range(early, NU):
        wait(sg.at[0, 0, pl.ds(0, 7)], sr_recv.at[u])
    send(sg.at[c, pl.ds(early, 2)], sg.at[c, pl.ds(early, 2)], s_send.at[7], sc_recv.at[1], mate)
    stage_g(6)
    stage_f(NU - 1)
    wait(sg.at[0, pl.ds(0, early)], sc_recv.at[0])
    wait(sg.at[0, pl.ds(0, 2)], sc_recv.at[1])

    m2 = m1f[...].reshape(NU * crow // 4, half)
    for o in range(8):
        for h in range(2):
            k = [mbuf[0, c, (2 * h + i) * 2 + o // 4, o % 4].reshape(crow, half)
                 for i in range(2)]
            m2 = m2 - jnp.dot(sg[h, :, o].reshape(NU * crow // 4, half),
                              jnp.concatenate(k, axis=0), preferred_element_type=F32)
    r = m2.astype(BF16)
    es[0, 0:1, :] = jnp.sum(m2 * r.astype(F32), axis=0, keepdims=True)
    share = crow // 4
    for u in range(NU):
        mbuf[1, c, u, x, zl] = r[u * share:(u + 1) * share]
    NP = 4

    def leg(p, k):
        at = pl.ds(2 * p, 2)
        if k == 0:
            return mbuf.at[1, c, at, x, zl], (zdev if p < NP - 1 else xdev)
        if p < NP - 1:
            return mbuf.at[1, c, at, x], xdev
        return mbuf.at[1, c, at, :, zl], zdev

    for p in range(NP):
        mine, to = leg(p, 0)
        for d in range(3):
            send(mine, mine, s_send.at[8], hz_recv.at[p], to[d])

    stage_g(NU - 1)
    step = 64

    def first(i, carry):
        at = pl.ds(pl.multiple_of(i * step, step), step)
        v = (st[at, :].astype(F32) - acc[at, :]).astype(BF16)
        psi1[at, :] = v
        w = v.astype(F32)
        n = jnp.sum(w * w, axis=1, keepdims=True)
        nrm[at, :] = jnp.broadcast_to(n, (step, half))
        return carry

    lax.fori_loop(0, rows // step, first, 0)
    for h in range(2):
        es[0, pl.ds(1 + h, 1), :] = nrm[pl.ds(h * half, half), :].T[0:1, :]
    for d in range(3):
        send(es.at[0], re.at[0, d], e_send.at[0], e_recv.at[0], zdev[d])
    for p in range(NP):
        wait(mbuf.at[0, 0, pl.ds(0, 2), 0, pl.ds(0, 3)], hz_recv.at[p])
        mine, to = leg(p, 1)
        for d in range(3):
            send(mine, mine, s_send.at[9], hx_recv.at[p], to[d])
    wait(re.at[0], e_recv.at[0])
    es[1] = es[0] + re[0, 0] + re[0, 1] + re[0, 2]
    for d in range(3):
        send(es.at[1], re.at[1, d], e_send.at[1], e_recv.at[1], xdev[d])

    def turn(p, h):
        for u in (2 * p, 2 * p + 1):
            m = mbuf[1, h, u].reshape(rows, half).astype(F32)
            mt2[pl.ds(pl.multiple_of(h * half, half), half), u * rows:(u + 1) * rows] = (
                m.T.astype(BF16))

    for p in range(NP):
        wait(mbuf.at[0, 0, pl.ds(0, 2), pl.ds(0, 3)], hx_recv.at[p])
        mine = mbuf.at[1, c, pl.ds(2 * p, 2)]
        send(mine, mine, s_send.at[10], hc_recv.at[p], mate)
        turn(p, c)
    wait(re.at[1], e_recv.at[1])
    es[2] = es[1] + re[1, 0] + re[1, 1] + re[1, 2]
    send(es.at[2], re.at[2, 0], e_send.at[2], e_recv.at[2], mate)
    for p in range(NP):
        wait(mbuf.at[0, 0, pl.ds(0, 2)], hc_recv.at[p])
        turn(p, 1 - c)

    def last(i, carry):
        at = pl.ds(pl.multiple_of(i * width, width), width)
        change = jnp.dot(mt2[...], wall[:, :, :, at].reshape(NU * rows, width),
                         preferred_element_type=F32)
        res[:, at] = (psi1[:, at].astype(F32) - change).astype(BF16)
        return carry

    lax.fori_loop(0, cols // width, last, 0)

    wait(re.at[2, 0], e_recv.at[2])
    mine, other = es[2, 0:1, :], re[2, 0, 0:1, :]
    norm = es[2, 1:3, :] + re[2, 0, 1:3, :]
    eout[0:1, :] = scale * jnp.where(c == 0, mine, other) / norm[0:1]
    eout[1:2, :] = scale * jnp.where(c == 0, other, mine) / norm[1:2]

    wait(wall.at[pl.ds(0, 4)], w_send.at[0])
    wait(wall.at[0], w_send.at[1])
    wait(wall.at[pl.ds(0, 2)], w_send.at[2])
    sizes = (rc, rx, rz, mbuf.at[0, 0, :, 0, pl.ds(0, 3)], mbuf.at[0, 0, :, pl.ds(0, 3)],
             mbuf.at[0, 0], sg.at[0, :, pl.ds(0, 7)], sg.at[0],
             mbuf.at[0, 0, :, 0, pl.ds(0, 3)], mbuf.at[0, 0, :, pl.ds(0, 3)], mbuf.at[0, 0])
    for k, ref in enumerate(sizes):
        wait(ref, s_send.at[k])
    wait(re.at[0], e_send.at[0])
    wait(re.at[1], e_send.at[1])
    wait(re.at[2, 0], e_send.at[2])


def per_device(orbitals, projectors):
    rows, cols = orbitals.shape
    half, crow = rows // 2, rows // CH
    share = crow // 4
    bands = rows * lax.axis_size("band")
    points = cols * lax.axis_size("grid")
    dma = pltpu.SemaphoreType.DMA
    vmem = pltpu.VMEM
    result, energies = pl.pallas_call(
        functools.partial(kernel, 2.0 * points / bands),
        out_shape=(pltpu.VMEM((rows, cols), BF16),
                   pltpu.VMEM((2, half), F32)),
        in_specs=[pl.BlockSpec(memory_space=pl.ANY)] * 2,
        out_specs=(pl.BlockSpec(memory_space=pltpu.VMEM),
                   pl.BlockSpec(memory_space=pltpu.VMEM)),
        scratch_shapes=[
            vmem((NU, 4, crow, cols), BF16),
            vmem((2 * rows, cols), BF16),
            vmem((rows, cols), BF16),
            vmem((rows, cols), F32),
            vmem((NU, rows, rows), BF16),
            vmem((NU, rows, rows), BF16),
            vmem((rows, rows), F32),
            vmem((NU, 4, crow, rows), BF16),
            vmem((2, 4, crow, rows), F32),
            vmem((NU, 3, crow, rows), BF16),
            vmem((NU, 4, share, rows), BF16),
            vmem((NU, 4, share, rows), F32),
            vmem((NU, 3, share, rows), BF16),
            vmem((NU, share, half), F32),
            vmem((2, 2, NU, 4, 4, share, half), BF16),
            vmem((2, NU, 8, share, half), BF16),
            vmem((rows, rows), BF16),
            vmem((rows, NU * rows), BF16),
            vmem((rows, half), F32),
            vmem((3, 8, half), F32),
            vmem((3, 3, 8, half), F32),
            dma((CH + 2,)),
            dma((3,)),
            dma((2, NU)),
            dma((NU,)),
            dma((NU,)),
            dma((CH,)),
            dma((11,)),
            dma((NU,)),
            dma((NU,)),
            dma((NU,)),
            dma((NU,)),
            dma((NU,)),
            dma((NU,)),
            dma((NU,)),
            dma((2,)),
            dma((4,)),
            dma((4,)),
            dma((4,)),
            dma((3,)),
            dma((3,)),
        ],
        compiler_params=pltpu.CompilerParams(
            collective_id=0, has_side_effects=True, vmem_limit_bytes=65_500_000),
    )(orbitals, projectors)
    return result, energies.reshape(rows)


def solution(mesh):
    in_specs = (P("band", "grid"), P("band", "grid"))
    out_specs = (P("band", "grid"), P("band"))
    return jax.shard_map(
        per_device, mesh=mesh, in_specs=in_specs, out_specs=out_specs, check_vma=False
    )
```

```python
import functools

import jax
import jax.numpy as jnp
from jax import lax
from jax.experimental import pallas as pl
from jax.experimental.pallas import tpu as pltpu
from jax.sharding import PartitionSpec as P

MESH = pl.DeviceIdType.MESH
F32, BF16 = jnp.float32, jnp.bfloat16
CH = 4
NU = 8
NT = (((1,), (1,)), ((), ()))


def kernel(scale, psi_hbm, w_hbm, res, eout, wall, st, psi1, acc,
           xs, rc, xown, sx, bs, rx, sz, zs, rz, m1f, mbuf, sg, mt, mt2, nrm, es, re,
           in_sem, w_send, n_recv, m_recv, f_recv, z_recv, s_send, c_recv, x_recv, zz_recv,
           gz_recv, gx_recv, gc_recv, sr_recv, sc_recv, hz_recv, hx_recv, hc_recv,
           e_send, e_recv):
    rows, cols = psi1.shape
    half = rows // 2
    crow = rows // CH
    b = lax.axis_index("band")
    g = lax.axis_index("grid")
    zh, y = b // 4, b % 4
    zl, x, c = g // 8, (g // 2) % 4, g % 2

    def dev(hh, yy, ll, xx, cc):
        return (hh * 4 + yy, (ll * 4 + xx) * 2 + cc)

    ym = [(y + d) % 4 for d in (1, 3, 2)]
    xm = [(x + d) % 4 for d in (2, 1, 3)]
    zm = [(zl + d) % 4 for d in (2, 1, 3)]
    ydev = [dev(zh, m, zl, x, c) for m in ym]
    odev = [dev(1 - zh, m, zl, x, c) for m in ym]
    right, left = ydev[0], ydev[1]
    zpart = dev(1 - zh, y, zl, x, c)
    mate = dev(zh, y, zl, x, 1 - c)
    xdev = [dev(zh, y, zl, m, c) for m in xm]
    zdev = [dev(zh, y, m, x, c) for m in zm]
    cross = [dev(zh, y, m, n, c) for m in zm for n in xm]
    bcore = [dev(1 - zh, m, zl, x, 1 - c) for m in ym + [y]] + [
        dev(zh, m, zl, x, 1 - c) for m in ym]

    def unit(t):
        return (t % 4) * 2 + (zh + t // 4) % 2

    def send(src, dst, ssem, rsem, to):
        pltpu.make_async_remote_copy(
            src_ref=src, dst_ref=dst, send_sem=ssem, recv_sem=rsem,
            device_id=to, device_id_type=MESH).start()

    def wait(ref, sem):
        pltpu.make_async_copy(ref, ref, sem).wait()

    barrier = pltpu.get_barrier_semaphore()
    peers = odev + [zpart] + bcore + cross + zdev + ydev + xdev + [mate]
    for p in peers:
        pl.semaphore_signal(barrier, inc=1, device_id=p, device_id_type=MESH)
    own = [wall.at[ch * 2 + zh, y] for ch in range(CH)]
    loads = [pltpu.make_async_copy(w_hbm.at[pl.ds(ch * crow, crow)], own[ch], in_sem.at[ch])
             for ch in range(CH)]
    loads.append(pltpu.make_async_copy(psi_hbm, st.at[pl.ds(0, rows)], in_sem.at[CH]))
    loads.append(pltpu.make_async_copy(w_hbm, st.at[pl.ds(rows, rows)], in_sem.at[CH + 1]))
    for load in loads:
        load.start()
    for load in loads[:CH]:
        load.wait()
    pl.semaphore_wait(barrier, len(peers))

    for ch in range(CH):
        send(own[ch], own[ch], w_send.at[1], z_recv.at[ch], zpart)

    hrow = crow // 2

    def near(k, kept):
        for side, to in ((0, right), (1, left)):
            part = wall.at[unit(k), y, pl.ds((side ^ kept) * hrow, hrow)]
            sem = m_recv.at[k] if kept else n_recv.at[side, k]
            send(part, part, w_send.at[0], sem, to)

    def pass_on(k):
        for side, m, to in ((0, (y + 3) % 4, right), (1, (y + 1) % 4, left)):
            wait(wall.at[0, 0, pl.ds(0, hrow)], n_recv.at[side, k])
            part = wall.at[unit(k), m, pl.ds(side * hrow, hrow)]
            send(part, part, w_send.at[2], f_recv.at[k], to)

        @pl.when(k + 1 < NU)
        def _():
            near(k + 1, 1)

        @pl.when((k + 2 >= CH) & (k + 2 < NU))
        def _():
            wait(wall.at[0, 0], z_recv.at[k + 2 - CH])

        @pl.when(k + 2 < NU)
        def _():
            near(k + 2, 0)

    near(0, 0)
    near(0, 1)
    near(1, 0)
    acc[...] = jnp.zeros_like(acc)
    es[...] = jnp.zeros_like(es)
    for load in loads[CH:]:
        load.wait()

    def stage_a(t):
        v = lax.dot_general(wall[unit(t)].reshape(rows, cols), st[...], NT,
                            preferred_element_type=F32)
        q = [v[:, i * half:(i + 1) * half] for i in range(4)]
        for i in range(2):
            at = slice(i * half, (i + 1) * half)
            xown[:, at] = jnp.where(c == 0, q[2 * i], q[2 * i + 1])
            xs[t, :, at] = jnp.where(c == 0, q[2 * i + 1], q[2 * i]).astype(BF16)
        send(xs.at[t], rc.at[t], s_send.at[0], c_recv.at[t], mate)

    def stage_b(t):
        wait(rc.at[t], c_recv.at[t])
        s = (xown[...] + rc[t].astype(F32)).reshape(4, crow, rows)
        bs[t % 2] = s
        sx[t] = s.astype(BF16)
        for d in range(3):
            send(sx.at[t, xm[d]], rx.at[t, d], s_send.at[1], x_recv.at[t], xdev[d])

    def stage_c(t):
        wait(rx.at[t], x_recv.at[t])
        s = bs[t % 2, x]
        for d in range(3):
            s = s + rx[t, d].astype(F32)
        s = s.reshape(4, crow // 4, rows)
        zs[t] = s
        sz[t] = s.astype(BF16)
        for d in range(3):
            send(sz.at[t, zm[d]], rz.at[t, d], s_send.at[2], zz_recv.at[t], zdev[d])

    def stage_d(t):
        wait(rz.at[t], zz_recv.at[t])
        s = zs[t, zl]
        for d in range(3):
            s = s + rz[t, d].astype(F32)
        u = unit(t)
        m1f[u] = s[:, :half]
        mine = mbuf.at[0, c, u, x, zl]
        mine[...] = s[:, :half].astype(BF16)
        sg[c, u, b] = s[:, half:].astype(BF16)
        last_unit = isinstance(t, int) and t == NU - 1
        if last_unit:
            spread(t)
        for to in cross + zdev + xdev if last_unit else zdev:
            send(mine, mine, s_send.at[12 if last_unit else 3], gz_recv.at[t], to)

    def spread(t):
        u = unit(t)
        mys = sg.at[c, u, b]
        for to in odev + [zpart] + ydev:
            send(mys, mys, s_send.at[6], sr_recv.at[u], to)

        def both_cores():
            for to in bcore + [mate]:
                send(mys, mys, s_send.at[11], sr_recv.at[u], to)

        if isinstance(t, int):
            if t % CH == CH - 1:
                both_cores()
        else:
            pl.when(t % CH == CH - 1)(both_cores)

    def stage_e(t):
        wait(mbuf.at[0, 0, 0, 0, pl.ds(0, 3)], gz_recv.at[t])
        mine = mbuf.at[0, c, unit(t), x]
        for d in range(3):
            send(mine, mine, s_send.at[4], gx_recv.at[t], xdev[d])

    def stage_f(t):
        wait(mbuf.at[0, 0, 0, pl.ds(0, 3)], gx_recv.at[t])
        mine = mbuf.at[0, c, unit(t)]
        send(mine, mine, s_send.at[5], gc_recv.at[t], mate)

    width = 512

    def stage_g(t):
        wait(mbuf.at[0, 0, 0], gc_recv.at[t])
        u = unit(t)
        for h in range(2):
            m = mbuf[0, h, u].reshape(rows, half).astype(F32)
            mt[pl.ds(h * half, half), :] = m.T.astype(BF16)

        def part(i, carry):
            at = pl.ds(pl.multiple_of(i * width, width), width)
            acc[:, at] += jnp.dot(mt[...], wall[u, :, :, at].reshape(rows, width),
                                  preferred_element_type=F32)
            return carry

        lax.fori_loop(0, cols // width, part, 0)

    late = 4

    def done(t):
        return jnp.where(t < late, 0, t - 1)

    def over(stage, lo, hi):
        def body(t, carry):
            stage(t)
            return carry

        lax.fori_loop(lo, hi, body, 0)

    def tick(n, carry):
        @pl.when(n < NU)
        def _():
            pass_on(n)

        t = n - 1

        @pl.when(t >= 0)
        def _():
            wait(wall.at[0, 0], m_recv.at[t])
            wait(wall.at[0, 0], f_recv.at[t])
            stage_a(t)

        @pl.when(t >= 0)
        def _():
            stage_b(t)

        @pl.when(t >= 1)
        def _():
            stage_c(t - 1)

        over(stage_d, done(t - 1), done(t))
        over(spread, done(t - 1), done(t))
        over(stage_e, done(t - 2), done(t - 1))
        over(stage_f, done(t - 3), done(t - 2))
        return carry

    lax.fori_loop(0, NU + 1, tick, 0)
    stage_g(0)
    stage_c(NU - 1)
    stage_e(NU - 3)
    stage_f(NU - 4)
    stage_g(1)
    stage_d(NU - 2)
    spread(NU - 2)
    stage_g(2)
    stage_d(NU - 1)
    stage_f(NU - 3)
    stage_g(3)
    stage_e(NU - 2)
    early = NU - 2
    for u in range(early):
        wait(sg.at[0, 0, pl.ds(0, 7)], sr_recv.at[u])
    send(sg.at[c, pl.ds(0, early)], sg.at[c, pl.ds(0, early)], s_send.at[7], sc_recv.at[0], mate)
    stage_g(4)
    stage_g(5)
    fifteen = mbuf.at[0, 0, pl.ds(0, 5), pl.ds(0, 3), 0]
    stage_f(NU - 2)
    wait(sg.at[0, pl.ds(0, early)], sc_recv.at[0])
    wait(fifteen, gz_recv.at[NU - 1])
    for u in range(early, NU):
        wait(fifteen, sr_recv.at[u])

    m2 = m1f[...].reshape(NU * crow // 4, half)
    for o in range(8):
        for h in range(2):
            k = [mbuf[0, c, (2 * h + i) * 2 + o // 4, o % 4].reshape(crow, half)
                 for i in range(2)]
            m2 = m2 - jnp.dot(sg[h, :, o].reshape(NU * crow // 4, half),
                              jnp.concatenate(k, axis=0), preferred_element_type=F32)
    r = m2.astype(BF16)
    es[0, 0:1, :] = jnp.sum(m2 * r.astype(F32), axis=0, keepdims=True)
    share = crow // 4
    for u in range(NU):
        mbuf[1, c, u, x, zl] = r[u * share:(u + 1) * share]
    NP = 4

    def leg(p, k):
        at = pl.ds(2 * p, 2)
        mine = [mbuf.at[1, c, at, x, zl]]
        if p < NP - 1:
            first, then = zdev, xdev
            others = [mbuf.at[1, c, at, x, m] for m in zm]
        else:
            first, then = xdev, zdev
            others = [mbuf.at[1, c, at, m, zl] for m in xm]
        return ((mine, first, 8, hz_recv), (mine, then, 9, hx_recv),
                (others, then, 9, hx_recv))[k]

    def go(p, k):
        parts, to, ssem, rsem = leg(p, k)
        for part in parts:
            for d in range(3):
                send(part, part, s_send.at[ssem], rsem.at[p], to[d])

    for p in range(NP):
        go(p, 0)
    for p in range(NP):
        go(p, 1)

    mine = mbuf.at[0, c, unit(NU - 1)]
    send(mine, mine, s_send.at[5], gc_recv.at[NU - 1], mate)
    stage_g(NU - 2)
    stage_g(NU - 1)
    step = 64

    def first(i, carry):
        at = pl.ds(pl.multiple_of(i * step, step), step)
        v = (st[at, :].astype(F32) - acc[at, :]).astype(BF16)
        psi1[at, :] = v
        w = v.astype(F32)
        n = jnp.sum(w * w, axis=1, keepdims=True)
        nrm[at, :] = jnp.broadcast_to(n, (step, half))
        return carry

    lax.fori_loop(0, rows // step, first, 0)
    for h in range(2):
        es[0, pl.ds(1 + h, 1), :] = nrm[pl.ds(h * half, half), :].T[0:1, :]
    for d in range(3):
        send(es.at[0], re.at[0, d], e_send.at[0], e_recv.at[0], zdev[d])
    for p in range(NP):
        wait(mbuf.at[0, 0, pl.ds(0, 2), 0, pl.ds(0, 3)], hz_recv.at[p])
        go(p, 2)
    wait(re.at[0], e_recv.at[0])
    es[1] = es[0] + re[0, 0] + re[0, 1] + re[0, 2]
    for d in range(3):
        send(es.at[1], re.at[1, d], e_send.at[1], e_recv.at[1], xdev[d])

    def turn(p, h):
        for u in (2 * p, 2 * p + 1):
            m = mbuf[1, h, u].reshape(rows, half).astype(F32)
            mt2[pl.ds(pl.multiple_of(h * half, half), half), u * rows:(u + 1) * rows] = (
                m.T.astype(BF16))

    for p in range(NP):
        wait(mbuf.at[0, 0, pl.ds(0, 2), pl.ds(0, 3)], hx_recv.at[p])
        mine = mbuf.at[1, c, pl.ds(2 * p, 2)]
        send(mine, mine, s_send.at[10], hc_recv.at[p], mate)
        turn(p, c)
    wait(re.at[1], e_recv.at[1])
    es[2] = es[1] + re[1, 0] + re[1, 1] + re[1, 2]
    send(es.at[2], re.at[2, 0], e_send.at[2], e_recv.at[2], mate)
    for p in range(NP):
        wait(mbuf.at[0, 0, pl.ds(0, 2)], hc_recv.at[p])
        turn(p, 1 - c)

    def last(i, carry):
        at = pl.ds(pl.multiple_of(i * width, width), width)
        change = jnp.dot(mt2[...], wall[:, :, :, at].reshape(NU * rows, width),
                         preferred_element_type=F32)
        res[:, at] = (psi1[:, at].astype(F32) - change).astype(BF16)
        return carry

    lax.fori_loop(0, cols // width, last, 0)

    wait(re.at[2, 0], e_recv.at[2])
    mine, other = es[2, 0:1, :], re[2, 0, 0:1, :]
    norm = es[2, 1:3, :] + re[2, 0, 1:3, :]
    eout[0:1, :] = scale * jnp.where(c == 0, mine, other) / norm[0:1]
    eout[1:2, :] = scale * jnp.where(c == 0, other, mine) / norm[1:2]

    wait(wall.at[pl.ds(0, 4)], w_send.at[0])
    wait(wall.at[0], w_send.at[1])
    wait(wall.at[pl.ds(0, 2)], w_send.at[2])
    most = pl.ds(0, NU - 1)
    sizes = (rc, rx, rz, mbuf.at[0, 0, most, 0, pl.ds(0, 3)], mbuf.at[0, 0, most, pl.ds(0, 3)],
             mbuf.at[0, 0], sg.at[0, :, pl.ds(0, 7)], sg.at[0, pl.ds(0, early)],
             mbuf.at[0, 0, :, 0, pl.ds(0, 3)], mbuf.at[0, 0, :, pl.ds(0, 3)], mbuf.at[0, 0],
             sg.at[0, pl.ds(0, 2)], fifteen)
    for k, ref in enumerate(sizes):
        wait(ref, s_send.at[k])
    wait(re.at[0], e_send.at[0])
    wait(re.at[1], e_send.at[1])
    wait(re.at[2, 0], e_send.at[2])


def per_device(orbitals, projectors):
    rows, cols = orbitals.shape
    half, crow = rows // 2, rows // CH
    share = crow // 4
    bands = rows * lax.axis_size("band")
    points = cols * lax.axis_size("grid")
    dma = pltpu.SemaphoreType.DMA
    vmem = pltpu.VMEM
    result, energies = pl.pallas_call(
        functools.partial(kernel, 2.0 * points / bands),
        out_shape=(pltpu.VMEM((rows, cols), BF16),
                   pltpu.VMEM((2, half), F32)),
        in_specs=[pl.BlockSpec(memory_space=pl.ANY)] * 2,
        out_specs=(pl.BlockSpec(memory_space=pltpu.VMEM),
                   pl.BlockSpec(memory_space=pltpu.VMEM)),
        scratch_shapes=[
            vmem((NU, 4, crow, cols), BF16),
            vmem((2 * rows, cols), BF16),
            vmem((rows, cols), BF16),
            vmem((rows, cols), F32),
            vmem((NU, rows, rows), BF16),
            vmem((NU, rows, rows), BF16),
            vmem((rows, rows), F32),
            vmem((NU, 4, crow, rows), BF16),
            vmem((2, 4, crow, rows), F32),
            vmem((NU, 3, crow, rows), BF16),
            vmem((NU, 4, share, rows), BF16),
            vmem((NU, 4, share, rows), F32),
            vmem((NU, 3, share, rows), BF16),
            vmem((NU, share, half), F32),
            vmem((2, 2, NU, 4, 4, share, half), BF16),
            vmem((2, NU, 8, share, half), BF16),
            vmem((rows, rows), BF16),
            vmem((rows, NU * rows), BF16),
            vmem((rows, half), F32),
            vmem((3, 8, half), F32),
            vmem((3, 3, 8, half), F32),
            dma((CH + 2,)),
            dma((3,)),
            dma((2, NU)),
            dma((NU,)),
            dma((NU,)),
            dma((CH,)),
            dma((13,)),
            dma((NU,)),
            dma((NU,)),
            dma((NU,)),
            dma((NU,)),
            dma((NU,)),
            dma((NU,)),
            dma((NU,)),
            dma((2,)),
            dma((4,)),
            dma((4,)),
            dma((4,)),
            dma((3,)),
            dma((3,)),
        ],
        compiler_params=pltpu.CompilerParams(
            collective_id=0, has_side_effects=True, vmem_limit_bytes=65_500_000),
    )(orbitals, projectors)
    return result, energies.reshape(rows)


def solution(mesh):
    in_specs = (P("band", "grid"), P("band", "grid"))
    out_specs = (P("band", "grid"), P("band"))
    return jax.shard_map(
        per_device, mesh=mesh, in_specs=in_specs, out_specs=out_specs, check_vma=False
    )
```

```python
import functools

import jax
import jax.numpy as jnp
from jax import lax
from jax.experimental import pallas as pl
from jax.experimental.pallas import tpu as pltpu
from jax.sharding import PartitionSpec as P

MESH = pl.DeviceIdType.MESH
F32, BF16 = jnp.float32, jnp.bfloat16
CH = 4
NU = 8
NT = (((1,), (1,)), ((), ()))


def kernel(scale, psi_hbm, w_hbm, res, eout, wall, st, psi1, acc,
           xs, rc, xown, sx, bs, rx, sz, zs, rz, m1f, mbuf, sg, mt, mt2, nrm, es, re,
           in_sem, w_send, n_recv, m_recv, f_recv, z_recv, s_send, c_recv, x_recv, zz_recv,
           gz_recv, gx_recv, gc_recv, sr_recv, sc_recv, hz_recv, hx_recv, hc_recv,
           e_send, e_recv):
    rows, cols = psi1.shape
    half = rows // 2
    crow = rows // CH
    b = lax.axis_index("band")
    g = lax.axis_index("grid")
    zh, y = b // 4, b % 4
    zl, x, c = g // 8, (g // 2) % 4, g % 2

    def dev(hh, yy, ll, xx, cc):
        return (hh * 4 + yy, (ll * 4 + xx) * 2 + cc)

    ym = [(y + d) % 4 for d in (1, 3, 2)]
    xm = [(x + d) % 4 for d in (2, 1, 3)]
    zm = [(zl + d) % 4 for d in (2, 1, 3)]
    ydev = [dev(zh, m, zl, x, c) for m in ym]
    odev = [dev(1 - zh, m, zl, x, c) for m in ym]
    right, left = ydev[0], ydev[1]
    zpart = dev(1 - zh, y, zl, x, c)
    mate = dev(zh, y, zl, x, 1 - c)
    xdev = [dev(zh, y, zl, m, c) for m in xm]
    zdev = [dev(zh, y, m, x, c) for m in zm]
    cross = [dev(zh, y, m, n, c) for m in zm for n in xm]
    bcore = [dev(1 - zh, m, zl, x, 1 - c) for m in ym + [y]] + [
        dev(zh, m, zl, x, 1 - c) for m in ym]

    def unit(t):
        return (t % 4) * 2 + (zh + t // 4) % 2

    def send(src, dst, ssem, rsem, to):
        pltpu.make_async_remote_copy(
            src_ref=src, dst_ref=dst, send_sem=ssem, recv_sem=rsem,
            device_id=to, device_id_type=MESH).start()

    def wait(ref, sem):
        pltpu.make_async_copy(ref, ref, sem).wait()

    barrier = pltpu.get_barrier_semaphore()
    peers = odev + [zpart] + bcore + cross + zdev + ydev + xdev + [mate]
    for p in peers:
        pl.semaphore_signal(barrier, inc=1, device_id=p, device_id_type=MESH)
    own = [wall.at[ch * 2 + zh, y] for ch in range(CH)]
    loads = [pltpu.make_async_copy(w_hbm.at[pl.ds(ch * crow, crow)], own[ch], in_sem.at[ch])
             for ch in range(CH)]
    loads.append(pltpu.make_async_copy(psi_hbm, st.at[pl.ds(0, rows)], in_sem.at[CH]))
    loads.append(pltpu.make_async_copy(w_hbm, st.at[pl.ds(rows, rows)], in_sem.at[CH + 1]))
    for load in loads:
        load.start()
    for load in loads[:CH]:
        load.wait()
    pl.semaphore_wait(barrier, len(peers))

    for ch in range(CH):
        send(own[ch], own[ch], w_send.at[1], z_recv.at[ch], zpart)

    hrow = crow // 2

    def near(k, kept):
        for side, to in ((0, right), (1, left)):
            part = wall.at[unit(k), y, pl.ds((side ^ kept) * hrow, hrow)]
            sem = m_recv.at[k] if kept else n_recv.at[side, k]
            send(part, part, w_send.at[0], sem, to)

    def pass_on(k):
        for side, m, to in ((0, (y + 3) % 4, right), (1, (y + 1) % 4, left)):
            wait(wall.at[0, 0, pl.ds(0, hrow)], n_recv.at[side, k])
            part = wall.at[unit(k), m, pl.ds(side * hrow, hrow)]
            send(part, part, w_send.at[2], f_recv.at[k], to)

        @pl.when(k + 1 < NU)
        def _():
            near(k + 1, 1)

        @pl.when((k + 2 >= CH) & (k + 2 < NU))
        def _():
            wait(wall.at[0, 0], z_recv.at[k + 2 - CH])

        @pl.when(k + 2 < NU)
        def _():
            near(k + 2, 0)

    near(0, 0)
    near(0, 1)
    near(1, 0)
    acc[...] = jnp.zeros_like(acc)
    es[...] = jnp.zeros_like(es)
    for load in loads[CH:]:
        load.wait()

    def stage_a(t):
        v = lax.dot_general(wall[unit(t)].reshape(rows, cols), st[...], NT,
                            preferred_element_type=F32)
        q = [v[:, i * half:(i + 1) * half] for i in range(4)]
        for i in range(2):
            at = slice(i * half, (i + 1) * half)
            xown[:, at] = jnp.where(c == 0, q[2 * i], q[2 * i + 1])
            xs[t, :, at] = jnp.where(c == 0, q[2 * i + 1], q[2 * i]).astype(BF16)
        send(xs.at[t], rc.at[t], s_send.at[0], c_recv.at[t], mate)

    def stage_b(t):
        wait(rc.at[t], c_recv.at[t])
        s = (xown[...] + rc[t].astype(F32)).reshape(4, crow, rows)
        bs[t % 2] = s
        sx[t] = s.astype(BF16)
        for d in range(3):
            send(sx.at[t, xm[d]], rx.at[t, d], s_send.at[1], x_recv.at[t], xdev[d])

    def stage_c(t):
        wait(rx.at[t], x_recv.at[t])
        s = bs[t % 2, x]
        for d in range(3):
            s = s + rx[t, d].astype(F32)
        s = s.reshape(4, crow // 4, rows)
        zs[t] = s
        sz[t] = s.astype(BF16)
        for d in range(3):
            send(sz.at[t, zm[d]], rz.at[t, d], s_send.at[2], zz_recv.at[t], zdev[d])

    def stage_d(t):
        wait(rz.at[t], zz_recv.at[t])
        s = zs[t, zl]
        for d in range(3):
            s = s + rz[t, d].astype(F32)
        u = unit(t)
        m1f[u] = s[:, :half]
        mine = mbuf.at[0, c, u, x, zl]
        mine[...] = s[:, :half].astype(BF16)
        sg[c, u, b] = s[:, half:].astype(BF16)
        last_unit = isinstance(t, int) and t == NU - 1
        if last_unit:
            spread(t)
        for to in cross + zdev + xdev if last_unit else zdev:
            send(mine, mine, s_send.at[12 if last_unit else 3], gz_recv.at[t], to)

    def spread(t):
        u = unit(t)
        mys = sg.at[c, u, b]
        for to in odev + [zpart] + ydev:
            send(mys, mys, s_send.at[6], sr_recv.at[u], to)

        def both_cores():
            for to in bcore + [mate]:
                send(mys, mys, s_send.at[11], sr_recv.at[u], to)

        if isinstance(t, int):
            if t % CH == CH - 1:
                both_cores()
        else:
            pl.when(t % CH == CH - 1)(both_cores)

    def stage_e(t):
        wait(mbuf.at[0, 0, 0, 0, pl.ds(0, 3)], gz_recv.at[t])
        mine = mbuf.at[0, c, unit(t), x]
        for d in range(3):
            send(mine, mine, s_send.at[4], gx_recv.at[t], xdev[d])

    def stage_f(t):
        wait(mbuf.at[0, 0, 0, pl.ds(0, 3)], gx_recv.at[t])
        mine = mbuf.at[0, c, unit(t)]
        send(mine, mine, s_send.at[5], gc_recv.at[t], mate)

    width = 512
    wide = 1024

    def stage_g(t):
        wait(mbuf.at[0, 0, 0], gc_recv.at[t])
        u = unit(t)
        for h in range(2):
            m = mbuf[0, h, u].reshape(rows, half).astype(F32)
            mt[pl.ds(h * half, half), :] = m.T.astype(BF16)

        def part(i, carry):
            at = pl.ds(pl.multiple_of(i * width, width), width)
            acc[:, at] += jnp.dot(mt[...], wall[u, :, :, at].reshape(rows, width),
                                  preferred_element_type=F32)
            return carry

        lax.fori_loop(0, cols // width, part, 0)

    late = 4

    def done(t):
        return jnp.where(t < late, 0, t - 1)

    def over(stage, lo, hi):
        def body(t, carry):
            stage(t)
            return carry

        lax.fori_loop(lo, hi, body, 0)

    def tick(n, carry):
        @pl.when(n < NU)
        def _():
            pass_on(n)

        t = n - 1

        over(stage_g, jnp.where(t == NU - 1, 0, 2), 2)

        @pl.when(t >= 0)
        def _():
            wait(wall.at[0, 0], m_recv.at[t])
            wait(wall.at[0, 0], f_recv.at[t])
            stage_a(t)

        @pl.when(t >= 0)
        def _():
            stage_b(t)

        @pl.when(t >= 1)
        def _():
            stage_c(t - 1)

        over(stage_d, done(t - 1), done(t))
        over(spread, done(t - 1), done(t))
        over(stage_e, done(t - 2), done(t - 1))
        over(stage_f, done(t - 3), done(t - 2))
        return carry

    lax.fori_loop(0, NU + 1, tick, 0)
    stage_c(NU - 1)
    stage_e(NU - 3)
    stage_f(NU - 4)
    stage_d(NU - 2)
    spread(NU - 2)
    stage_g(2)
    stage_d(NU - 1)
    stage_f(NU - 3)
    stage_g(3)
    stage_e(NU - 2)
    early = NU - 2
    for u in range(early):
        wait(sg.at[0, 0, pl.ds(0, 7)], sr_recv.at[u])
    send(sg.at[c, pl.ds(0, early)], sg.at[c, pl.ds(0, early)], s_send.at[7], sc_recv.at[0], mate)
    stage_g(4)
    stage_g(5)
    fifteen = mbuf.at[0, 0, pl.ds(0, 5), pl.ds(0, 3), 0]
    stage_f(NU - 2)
    wait(sg.at[0, pl.ds(0, early)], sc_recv.at[0])
    wait(fifteen, gz_recv.at[NU - 1])
    for u in range(early, NU):
        wait(fifteen, sr_recv.at[u])

    m2 = m1f[...].reshape(NU * crow // 4, half)
    for o in range(8):
        for h in range(2):
            k = [mbuf[0, c, (2 * h + i) * 2 + o // 4, o % 4].reshape(crow, half)
                 for i in range(2)]
            m2 = m2 - jnp.dot(sg[h, :, o].reshape(NU * crow // 4, half),
                              jnp.concatenate(k, axis=0), preferred_element_type=F32)
    r = m2.astype(BF16)
    es[0, 0:1, :] = jnp.sum(m2 * r.astype(F32), axis=0, keepdims=True)
    share = crow // 4
    for u in range(NU):
        mbuf[1, c, u, x, zl] = r[u * share:(u + 1) * share]
    NP = 4

    def leg(p, k):
        at = pl.ds(2 * p, 2)
        mine = [mbuf.at[1, c, at, x, zl]]
        if p < NP - 1:
            first, then = zdev, xdev
            others = [mbuf.at[1, c, at, x, m] for m in zm]
        else:
            first, then = xdev, zdev
            others = [mbuf.at[1, c, at, m, zl] for m in xm]
        return ((mine, first, 8, hz_recv), (mine, then, 9, hx_recv),
                (others, then, 9, hx_recv))[k]

    def go(p, k):
        parts, to, ssem, rsem = leg(p, k)
        for part in parts:
            for d in range(3):
                send(part, part, s_send.at[ssem], rsem.at[p], to[d])

    for p in range(NP):
        go(p, 0)
    for p in range(NP):
        go(p, 1)

    mine = mbuf.at[0, c, unit(NU - 1)]
    send(mine, mine, s_send.at[5], gc_recv.at[NU - 1], mate)
    stage_g(NU - 2)
    stage_g(NU - 1)
    step = 64

    def first(i, carry):
        at = pl.ds(pl.multiple_of(i * step, step), step)
        v = (st[at, :].astype(F32) - acc[at, :]).astype(BF16)
        psi1[at, :] = v
        w = v.astype(F32)
        n = jnp.sum(w * w, axis=1, keepdims=True)
        nrm[at, :] = jnp.broadcast_to(n, (step, half))
        return carry

    lax.fori_loop(0, rows // step, first, 0)
    for h in range(2):
        es[0, pl.ds(1 + h, 1), :] = nrm[pl.ds(h * half, half), :].T[0:1, :]
    for d in range(3):
        send(es.at[0], re.at[0, d], e_send.at[0], e_recv.at[0], zdev[d])
    for p in range(NP):
        wait(mbuf.at[0, 0, pl.ds(0, 2), 0, pl.ds(0, 3)], hz_recv.at[p])
        go(p, 2)
    wait(re.at[0], e_recv.at[0])
    es[1] = es[0] + re[0, 0] + re[0, 1] + re[0, 2]
    for d in range(3):
        send(es.at[1], re.at[1, d], e_send.at[1], e_recv.at[1], xdev[d])

    def turn(p, h):
        for u in (2 * p, 2 * p + 1):
            m = mbuf[1, h, u].reshape(rows, half).astype(F32)
            mt2[pl.ds(pl.multiple_of(h * half, half), half), u * rows:(u + 1) * rows] = (
                m.T.astype(BF16))

    for p in range(NP):
        wait(mbuf.at[0, 0, pl.ds(0, 2), pl.ds(0, 3)], hx_recv.at[p])
        mine = mbuf.at[1, c, pl.ds(2 * p, 2)]
        send(mine, mine, s_send.at[10], hc_recv.at[p], mate)
        turn(p, c)
    wait(re.at[1], e_recv.at[1])
    es[2] = es[1] + re[1, 0] + re[1, 1] + re[1, 2]
    send(es.at[2], re.at[2, 0], e_send.at[2], e_recv.at[2], mate)
    for p in range(NP):
        wait(mbuf.at[0, 0, pl.ds(0, 2)], hc_recv.at[p])
        turn(p, 1 - c)

    def last(i, carry):
        at = pl.ds(pl.multiple_of(i * wide, wide), wide)
        change = jnp.dot(mt2[...], wall[:, :, :, at].reshape(NU * rows, wide),
                         preferred_element_type=F32)
        res[:, at] = (psi1[:, at].astype(F32) - change).astype(BF16)
        return carry

    lax.fori_loop(0, cols // wide, last, 0)

    wait(re.at[2, 0], e_recv.at[2])
    mine, other = es[2, 0:1, :], re[2, 0, 0:1, :]
    norm = es[2, 1:3, :] + re[2, 0, 1:3, :]
    eout[0:1, :] = scale * jnp.where(c == 0, mine, other) / norm[0:1]
    eout[1:2, :] = scale * jnp.where(c == 0, other, mine) / norm[1:2]

    wait(wall.at[pl.ds(0, 4)], w_send.at[0])
    wait(wall.at[0], w_send.at[1])
    wait(wall.at[pl.ds(0, 2)], w_send.at[2])
    most = pl.ds(0, NU - 1)
    sizes = (rc, rx, rz, mbuf.at[0, 0, most, 0, pl.ds(0, 3)], mbuf.at[0, 0, most, pl.ds(0, 3)],
             mbuf.at[0, 0], sg.at[0, :, pl.ds(0, 7)], sg.at[0, pl.ds(0, early)],
             mbuf.at[0, 0, :, 0, pl.ds(0, 3)], mbuf.at[0, 0, :, pl.ds(0, 3)], mbuf.at[0, 0],
             sg.at[0, pl.ds(0, 2)], fifteen)
    for k, ref in enumerate(sizes):
        wait(ref, s_send.at[k])
    wait(re.at[0], e_send.at[0])
    wait(re.at[1], e_send.at[1])
    wait(re.at[2, 0], e_send.at[2])


def per_device(orbitals, projectors):
    rows, cols = orbitals.shape
    half, crow = rows // 2, rows // CH
    share = crow // 4
    bands = rows * lax.axis_size("band")
    points = cols * lax.axis_size("grid")
    dma = pltpu.SemaphoreType.DMA
    vmem = pltpu.VMEM
    result, energies = pl.pallas_call(
        functools.partial(kernel, 2.0 * points / bands),
        out_shape=(pltpu.VMEM((rows, cols), BF16),
                   pltpu.VMEM((2, half), F32)),
        in_specs=[pl.BlockSpec(memory_space=pl.ANY)] * 2,
        out_specs=(pl.BlockSpec(memory_space=pltpu.VMEM),
                   pl.BlockSpec(memory_space=pltpu.VMEM)),
        scratch_shapes=[
            vmem((NU, 4, crow, cols), BF16),
            vmem((2 * rows, cols), BF16),
            vmem((rows, cols), BF16),
            vmem((rows, cols), F32),
            vmem((NU, rows, rows), BF16),
            vmem((NU, rows, rows), BF16),
            vmem((rows, rows), F32),
            vmem((NU, 4, crow, rows), BF16),
            vmem((2, 4, crow, rows), F32),
            vmem((NU, 3, crow, rows), BF16),
            vmem((NU, 4, share, rows), BF16),
            vmem((NU, 4, share, rows), F32),
            vmem((NU, 3, share, rows), BF16),
            vmem((NU, share, half), F32),
            vmem((2, 2, NU, 4, 4, share, half), BF16),
            vmem((2, NU, 8, share, half), BF16),
            vmem((rows, rows), BF16),
            vmem((rows, NU * rows), BF16),
            vmem((rows, half), F32),
            vmem((3, 8, half), F32),
            vmem((3, 3, 8, half), F32),
            dma((CH + 2,)),
            dma((3,)),
            dma((2, NU)),
            dma((NU,)),
            dma((NU,)),
            dma((CH,)),
            dma((13,)),
            dma((NU,)),
            dma((NU,)),
            dma((NU,)),
            dma((NU,)),
            dma((NU,)),
            dma((NU,)),
            dma((NU,)),
            dma((2,)),
            dma((4,)),
            dma((4,)),
            dma((4,)),
            dma((3,)),
            dma((3,)),
        ],
        compiler_params=pltpu.CompilerParams(
            collective_id=0, has_side_effects=True, vmem_limit_bytes=65_500_000),
    )(orbitals, projectors)
    return result, energies.reshape(rows)


def solution(mesh):
    in_specs = (P("band", "grid"), P("band", "grid"))
    out_specs = (P("band", "grid"), P("band"))
    return jax.shard_map(
        per_device, mesh=mesh, in_specs=in_specs, out_specs=out_specs, check_vma=False
    )
```
